8 devices in a mesh: dp: 1 (over z), dcp: 8 (over y, x, core).
Axes of the slice: x: 2, y: 2, z: 1, core: 2. Of those that a mesh axis runs over, the one named last changes fastest.
Arguments:
- q: bfloat16 [128, 64, 576], P('dp', 'dcp')
- cache: bfloat16 [128, 128, 8, 8, 576], P('dp', None, 'dcp')
- lens: int32 [128], P('dp')
Outputs:
- output: bfloat16 [128, 64, 512], P('dp', 'dcp')
All inputs are finite; a program needn't handle non-finite values.
Results may differ from the reference program's by a relative error of at most 0.00740601.
Values are sent between devices in bfloat16 or wider.
A program may use at most 1 GiB of HBM per device.

```python
import jax
import jax.numpy as jnp
from jax import lax

B = 128
S = 8192
PAGE = 8
DCP = 8
HEADS = 64
LORA = 512
ROPE = 64
NOPE = 128

R = S // (PAGE * DCP)
K = LORA + ROPE


def setup_inputs(seed: int = 0, part: int = 0) -> dict:
    key = jax.random.fold_in(jax.random.key(seed), part)
    kq, kc, kl = jax.random.split(key, 3)
    qs = 1.5 * ((NOPE + ROPE) / 2.0) ** 0.5
    scale = jnp.concatenate([jnp.full((LORA,), qs / LORA ** 0.5, jnp.float32), jnp.full((ROPE,), qs / ROPE ** 0.5, jnp.float32)])
    q = (jax.random.normal(kq, (B, HEADS, K), jnp.float32) * scale).astype(jnp.bfloat16)
    cache = jax.random.normal(kc, (B, R, DCP, PAGE, K), jnp.float32).astype(jnp.bfloat16)
    lens = jax.random.randint(kl, (B,), S // 4, S + 1, jnp.int32)
    return {'q': q, 'cache': cache, 'lens': lens}


def reference(q, cache, lens):
    c = cache.reshape(B, S, K)
    pos = jnp.arange(S)

    def one(args):
        qb, cb, lb = args
        s = jnp.dot(qb, cb.T, preferred_element_type=jnp.float32) / (NOPE + ROPE) ** 0.5
        s = jnp.where(pos[None, :] < lb, s, -jnp.inf)
        a = jax.nn.softmax(s, axis=1)
        o = jnp.dot(a, cb[:, :LORA].astype(jnp.float32), preferred_element_type=jnp.float32)
        return o.astype(jnp.bfloat16)

    return lax.map(one, (q, c, lens))
```

```python
import functools

import jax
import jax.numpy as jnp
from jax import lax
from jax.experimental import pallas as pl
from jax.experimental.pallas import tpu as pltpu
from jax.sharding import PartitionSpec as P

ROPE = 64
QK_DIM = 192
SCALE = QK_DIM ** -0.5
MESH = pl.DeviceIdType.MESH

G = 8
PAIRS = G // 2
AHEAD = 4
LAG1, LAG2, LAG3 = 6, 14, 22
NBUF = 6
AG_KINDS, RS_KINDS = 7, 6


def attend(q, c, length, d, lora):
    heads = q.shape[0]
    slots, k, pages = c.shape
    lane = lax.broadcasted_iota(jnp.int32, (heads, pages), 1)
    s = []
    for i in range(0, slots, 2):
        both = jnp.concatenate([c[i], c[i + 1]], axis=1)
        dots = jnp.dot(q, both, preferred_element_type=jnp.float32)
        for u in range(2):
            n = lax.shift_right_arithmetic(length - slots * d - (i + u) + (slots * 8 - 1), 6)
            s.append(jnp.where(lane < n, dots[:, pages * u:pages * (u + 1)] * SCALE, -jnp.inf))
    m = jnp.max(functools.reduce(jnp.maximum, s), axis=1, keepdims=True)
    m = jnp.where(m == -jnp.inf, 0.0, m)
    p = [jnp.exp(x - m) for x in s]
    l = jnp.sum(functools.reduce(jnp.add, p), axis=1, keepdims=True)
    o = None
    for i in range(0, slots, 2):
        pb = jnp.concatenate([p[i], p[i + 1]], axis=1).astype(jnp.bfloat16)
        both = jnp.concatenate([c[i, :lora], c[i + 1, :lora]], axis=1)
        x = lax.dot_general(pb, both, (((1,), (1,)), ((), ())), preferred_element_type=jnp.float32)
        o = x if o is None else o + x
    has = l > 0.0
    r = jnp.where(has, 1.0 / jnp.where(has, l, 1.0), 0.0)
    lse = jnp.where(has, m + jnp.log(jnp.where(has, l, 1.0)), -jnp.inf)
    return (o * r).astype(jnp.bfloat16), lse


def column(ref, lane, j):
    return jnp.max(jnp.where(lane == j, ref, -jnp.inf), axis=1, keepdims=True)


def merge(oa, la, ob, lb):
    top = jnp.maximum(la, lb)
    top = jnp.where(top == -jnp.inf, 0.0, top)
    wa, wb = jnp.exp(la - top), jnp.exp(lb - top)
    w = wa + wb
    has = w > 0.0
    safe = jnp.where(has, w, 1.0)
    inv = jnp.where(has, 1.0 / safe, 0.0)
    o = (wa * inv) * oa.astype(jnp.float32) + (wb * inv) * ob.astype(jnp.float32)
    return o.astype(jnp.bfloat16), jnp.where(has, top + jnp.log(safe), -jnp.inf)


def kernel(n_seq, lora, lens_ref, q_ref, c_ref, out_ref, kv, qg, o, lse, r1, rl1, r2, rl2, r3, rl3,
           kv_sem, q_sem, send_sem, recv_sem):
    n_groups, n_pairs = n_seq // G, n_seq // 2
    off_pair, off_group = LAG3 + 2, (LAG3 + 2) // PAIRS
    me = lax.axis_index("dcp")
    dp = lax.axis_index("dp")
    y, x, core = me // 4, (me // 2) % 2, me % 2
    partner = (dp, y * 4 + x * 2 + (1 - core))

    def neighbour(g, first):
        par = g % 2 if first else (g + 1) % 2
        return (dp, ((y + par) % 2) * 4 + ((x + 1 - par) % 2) * 2 + core)

    def remote(kind, g, src, dst, device):
        return pltpu.make_async_remote_copy(
            src_ref=src, dst_ref=dst, send_sem=send_sem.at[kind, g], recv_sem=recv_sem.at[kind, g],
            device_id=device, device_id_type=MESH)

    def q_block(g, block):
        return qg.at[pl.ds(g * G, G), pl.ds(block * 8, 8)]

    def q_copy(kind, g):
        src, dst, to = ((0, 4, partner), (0, 2, neighbour(g, True)), (0, 1, neighbour(g, False)),
                        (2, 3, neighbour(g, False)), (2, 6, partner), (1, 5, partner), (3, 7, partner))[kind]
        return remote(kind, g, q_block(g, src), q_block(g, dst), to)

    def seqs(ref, g, lo, hi):
        return ref.at[pl.ds((g + off_group) * G, G), pl.ds(lo, hi - lo)]

    def rs_copies(stage, g):
        rows, dst, ldst, to = ((32, r1, rl1, partner), (16, r2, rl2, neighbour(g, True)),
                               (8, r3, rl3, neighbour(g, False)))[stage]
        kind = AG_KINDS + 2 * stage
        return (remote(kind, g, seqs(o, g, rows, 2 * rows), seqs(dst, g, 0, rows), to),
                remote(kind + 1, g, lse.at[g + off_group, pl.ds(rows, rows)], ldst.at[g + off_group], to))

    def start_own(g):
        for kind in (0, 1, 2):
            q_copy(kind, g).start()

    def forward(g):
        q_copy(1, g).wait_recv()
        q_copy(2, g).wait_recv()
        for kind in (3, 4, 5):
            q_copy(kind, g).start()

    def forward_diagonal(g):
        q_copy(3, g).wait_recv()
        q_copy(6, g).start()

    def q_ready(g):
        for kind in (0, 4, 5, 6):
            q_copy(kind, g).wait_recv()

    def rs_start(stage, g):
        for copy in rs_copies(stage, g):
            copy.start()

    def rs_wait(stage, g):
        for copy in rs_copies(stage, g):
            copy.wait_recv()

    def kv_copy(b):
        slot = b % NBUF
        return pltpu.make_async_copy(c_ref.at[b], kv.at[slot], kv_sem.at[slot])

    for b in range(NBUF - 2):
        kv_copy(b).start()
    own = pltpu.make_async_copy(q_ref, qg.at[:, pl.ds(0, 8)], q_sem)
    own.start()

    barrier = pltpu.get_barrier_semaphore()
    for device in (partner, neighbour(0, True), neighbour(0, False)):
        pl.semaphore_signal(barrier, inc=1, device_id=device, device_id_type=MESH)
    pl.semaphore_wait(barrier, 3)
    own.wait()

    for g in range(AHEAD):
        start_own(g)
    forward(0)
    forward(1)
    forward_diagonal(0)

    lane = lax.broadcasted_iota(jnp.int32, (8 * 8, 128), 1)

    def combine(stage, pair):
        rows, ref, lref = ((32, r1, rl1), (16, r2, rl2), (8, r3, rl3))[stage]
        g = pair // PAIRS
        for u in range(2):
            b = 2 * pair + u
            j = b % G
            mine = lse[g, 0:rows]
            merged, total = merge(o[b, 0:rows], column(mine, lane[0:rows], j),
                                  ref[b], column(lref[g], lane[0:rows], j))
            if stage == 2:
                out_ref[jnp.maximum(b - 2 * off_pair, 0)] = merged
            else:
                o[b, 0:rows] = merged
                lse[g, 0:rows] = jnp.where(lane[0:rows] == j, total, mine)

    def attention(t):
        for u in range(2):
            b = 2 * t + u
            part, total = attend(qg[b], kv.at[b % NBUF], lens_ref[b], me, lora)
            o[b + 2 * off_pair] = part
            g = t // PAIRS + off_group
            lse[g] = jnp.where(lane == b % G, total, lse[g])

    def step(t, _):
        g = t // PAIRS

        @pl.when(t % PAIRS == 0)
        def _():
            @pl.when(g + AHEAD < n_groups)
            def _():
                start_own(g + AHEAD)

            @pl.when(g + 2 < n_groups)
            def _():
                forward(g + 2)

            @pl.when(g + 1 < n_groups)
            def _():
                forward_diagonal(g + 1)

            q_ready(g)

            @pl.when(g >= 1)
            def _():
                rs_start(0, g - 1)

        @pl.when(t % PAIRS == 2)
        def _():
            @pl.when(g >= 1)
            def _():
                rs_wait(0, g - 1)

            @pl.when(g >= 2)
            def _():
                rs_start(1, g - 2)

            @pl.when(g >= 3)
            def _():
                rs_wait(1, g - 3)

            @pl.when(g >= 4)
            def _():
                rs_start(2, g - 4)

            @pl.when(g >= 5)
            def _():
                rs_wait(2, g - 5)

        @pl.when(t + NBUF // 2 - 1 < n_pairs)
        def _():
            for u in range(2):
                kv_copy(2 * t + NBUF - 2 + u).start()
        for u in range(2):
            kv_copy(2 * t + u).wait()
        combine(0, t - LAG1 + off_pair)
        combine(1, t - LAG2 + off_pair)
        combine(2, t - LAG3 + off_pair)
        attention(t)
        return 0

    lax.fori_loop(0, n_pairs, step, 0)

    def combine_all(stage, lo, hi):
        def one(t, _):
            combine(stage, t + off_pair)
            return 0
        lax.fori_loop(lo, hi, one, 0)

    last = n_groups - 1
    rs_start(0, last)
    combine_all(0, n_pairs - LAG1, n_pairs - PAIRS)
    rs_start(1, last - 1)
    combine_all(1, n_pairs - LAG2, n_pairs - LAG2 + 2)
    rs_start(2, last - 3)
    rs_wait(1, last - 2)
    combine_all(1, n_pairs - 3 * PAIRS, n_pairs - 2 * PAIRS)
    rs_start(2, last - 2)
    rs_wait(0, last)
    combine_all(0, n_pairs - PAIRS, n_pairs)
    rs_start(1, last)
    rs_wait(2, last - 4)
    combine_all(2, n_pairs - LAG3, n_pairs - 4 * PAIRS)
    rs_wait(1, last - 1)
    combine_all(1, n_pairs - 2 * PAIRS, n_pairs - PAIRS)
    rs_start(2, last - 1)
    rs_wait(2, last - 3)
    combine_all(2, n_pairs - 4 * PAIRS, n_pairs - 3 * PAIRS)
    rs_wait(1, last)
    combine_all(1, n_pairs - PAIRS, n_pairs)
    rs_start(2, last)
    rs_wait(2, last - 2)
    combine_all(2, n_pairs - 3 * PAIRS, n_pairs - 2 * PAIRS)
    rs_wait(2, last - 1)
    combine_all(2, n_pairs - 2 * PAIRS, n_pairs - PAIRS)

    def sent(g, _):
        for kind in range(AG_KINDS):
            q_copy(kind, g).wait_send()
        for stage in range(3):
            for copy in rs_copies(stage, g):
                copy.wait_send()
        return 0

    lax.fori_loop(0, n_groups, sent, 0)
    rs_wait(2, last)
    combine_all(2, n_pairs - PAIRS, n_pairs)


def solution(mesh):
    def local(lens, q, cache):
        b, heads, k = q.shape
        r, page = cache.shape[1], cache.shape[3]
        lora = k - ROPE
        c = jnp.transpose(cache.reshape(b, r, page, k), (0, 2, 3, 1))
        groups = b // G
        off_group = (LAG3 + 2) // PAIRS
        pb = b + off_group * G
        pg = groups + off_group
        bf, f4 = jnp.bfloat16, jnp.float32
        kinds = AG_KINDS + RS_KINDS
        return pl.pallas_call(
            functools.partial(kernel, b, lora),
            out_shape=jax.ShapeDtypeStruct((b, heads, lora), bf),
            in_specs=[pl.BlockSpec(memory_space=pltpu.SMEM), pl.BlockSpec(memory_space=pl.ANY),
                      pl.BlockSpec(memory_space=pl.ANY)],
            out_specs=pl.BlockSpec(memory_space=pltpu.VMEM),
            scratch_shapes=[
                pltpu.VMEM((NBUF, page, k, r), bf),
                pltpu.VMEM((b, 8 * heads, k), bf),
                pltpu.VMEM((pb, 64, lora), bf), pltpu.VMEM((pg, 64, 128), f4),
                pltpu.VMEM((pb, 32, lora), bf), pltpu.VMEM((pg, 32, 128), f4),
                pltpu.VMEM((pb, 16, lora), bf), pltpu.VMEM((pg, 16, 128), f4),
                pltpu.VMEM((pb, 8, lora), bf), pltpu.VMEM((pg, 8, 128), f4),
                pltpu.SemaphoreType.DMA((NBUF,)), pltpu.SemaphoreType.DMA,
                pltpu.SemaphoreType.DMA((kinds, groups)), pltpu.SemaphoreType.DMA((kinds, groups)),
            ],
            compiler_params=pltpu.CompilerParams(collective_id=0, has_side_effects=True,
                                                 vmem_limit_bytes=64 * 2 ** 20 - 2 ** 16),
            name="decode",
        )(lens, q, c)

    f = jax.shard_map(local, mesh=mesh, in_specs=(P('dp'), P('dp', 'dcp', None), P('dp', None, 'dcp', None, None)),
                      out_specs=P('dp', 'dcp', None), check_vma=False)
    return lambda q, cache, lens: f(lens, q, cache)
```

```python
import functools

import jax
import jax.numpy as jnp
from jax import lax
from jax.experimental import pallas as pl
from jax.experimental.pallas import tpu as pltpu
from jax.sharding import PartitionSpec as P

ROPE = 64
QK_DIM = 192
SCALE = QK_DIM ** -0.5
MESH = pl.DeviceIdType.MESH

G = 8
W = 4
UNITS = G // W
AHEAD = 4
LAG1, LAG2, LAG3 = 4, 10, 16
OFF = 16
NBUF = 3 * W
TILE = 256
LOG2E = 1.4426950408889634
AG_KINDS, RS_KINDS = 14, 6


def scores(ql, r, c):
    lora = 2 * TILE
    heads, rope = r.shape

    def rows(p, lo, hi):
        return jnp.concatenate([c[2 * p, lo:hi], c[2 * p + 1, lo:hi]], axis=1)

    ql = jnp.concatenate([ql] * 2, axis=0)
    z = jnp.zeros((heads, rope), jnp.bfloat16)
    qr = jnp.concatenate([jnp.concatenate([r if i == p else z for i in range(4)], axis=1)
                          for p in range(4)], axis=0)
    cr = jnp.concatenate([rows(p, lora, lora + rope) for p in range(4)], axis=0)
    rotary = jnp.dot(qr, cr, preferred_element_type=jnp.float32)
    out = []
    for p in range(4):
        v = jnp.dot(ql, rows(p, 0, lora), preferred_element_type=jnp.float32)[:heads]
        v = v + rotary[heads * p:heads * (p + 1)]
        out += [v[:, :128], v[:, 128:]]
    return out


def values(p, c):
    lora = 2 * TILE
    o = None
    for i in range(4):
        both = jnp.concatenate([c[2 * i, :lora], c[2 * i + 1, :lora]], axis=1)
        x = lax.dot_general(p[i], both, (((1,), (1,)), ((), ())), preferred_element_type=jnp.float32)
        o = x if o is None else o + x
    return o.astype(jnp.bfloat16)


def softmax(s, length, d):
    lane = lax.broadcasted_iota(jnp.int32, s[0].shape, 1)
    s = [jnp.where(lane < lax.shift_right_arithmetic(length - 8 * d - i + 63, 6), v, -jnp.inf)
         for i, v in enumerate(s)]
    m = jnp.max(functools.reduce(jnp.maximum, s), axis=1, keepdims=True)
    m = jnp.where(m == -jnp.inf, 0.0, m)
    mc = m * (SCALE * LOG2E)
    p = [jnp.exp2(v * (SCALE * LOG2E) - mc) for v in s]
    l = jnp.sum(functools.reduce(jnp.add, p), axis=1, keepdims=True)
    has = l > 0.0
    safe = jnp.where(has, l, 1.0)
    r = jnp.where(has, 1.0 / safe, 0.0)
    lse = jnp.where(has, m * SCALE + jnp.log(safe), -jnp.inf)
    return [jnp.concatenate([p[2 * i] * r, p[2 * i + 1] * r], axis=1).astype(jnp.bfloat16) for i in range(4)], lse


def column(ref, lane, j):
    return jnp.max(jnp.where(lane == j, ref, -jnp.inf), axis=1, keepdims=True)


def merge(oa, la, ob, lb):
    top = jnp.maximum(la, lb)
    top = jnp.where(top == -jnp.inf, 0.0, top)
    wa, wb = jnp.exp(la - top), jnp.exp(lb - top)
    w = wa + wb
    has = w > 0.0
    safe = jnp.where(has, w, 1.0)
    inv = jnp.where(has, 1.0 / safe, 0.0)
    o = (wa * inv) * oa.astype(jnp.float32) + (wb * inv) * ob.astype(jnp.float32)
    return o.astype(jnp.bfloat16), jnp.where(has, top + jnp.log(safe), -jnp.inf)


def kernel(n_seq, lora, lens_ref, ql_ref, qr_ref, c_ref, out_ref, kv, ql, qr, prob, o, lse, r1, rl1, r2, rl2, r3, rl3,
           kv_sem, q_sem, send_sem, recv_sem):
    n_groups, n_units = n_seq // G, n_seq // W
    off_group = OFF // UNITS
    me = lax.axis_index("dcp")
    dp = lax.axis_index("dp")
    y, x, core = me // 4, (me // 2) % 2, me % 2
    partner = (dp, y * 4 + x * 2 + (1 - core))

    def neighbour(g, first):
        par = g % 2 if first else (g + 1) % 2
        return (dp, ((y + par) % 2) * 4 + ((x + 1 - par) % 2) * 2 + core)

    def remote(kind, g, src, dst, device):
        return pltpu.make_async_remote_copy(
            src_ref=src, dst_ref=dst, send_sem=send_sem.at[kind, g], recv_sem=recv_sem.at[kind, g],
            device_id=device, device_id_type=MESH)

    def q_blocks(g, block):
        return (ql.at[pl.ds(g * G, G), pl.ds(block * 8, 8)], qr.at[pl.ds(g * G // 2, G // 2), pl.ds(block * 8, 8)])

    def q_copies(kind, g):
        src, dst, to = ((0, 4, partner), (0, 2, neighbour(g, True)), (0, 1, neighbour(g, False)),
                        (2, 3, neighbour(g, False)), (2, 6, partner), (1, 5, partner), (3, 7, partner))[kind]
        return [remote(2 * kind + i, g, q_blocks(g, src)[i], q_blocks(g, dst)[i], to) for i in range(2)]

    def seqs(ref, g, lo, hi):
        return ref.at[pl.ds((g + off_group) * G, G), pl.ds(lo, hi - lo)]

    def rs_copies(stage, g):
        rows, dst, ldst, to = ((32, r1, rl1, partner), (16, r2, rl2, neighbour(g, True)),
                               (8, r3, rl3, neighbour(g, False)))[stage]
        kind = AG_KINDS + 2 * stage
        return (remote(kind, g, seqs(o, g, rows, 2 * rows), seqs(dst, g, 0, rows), to),
                remote(kind + 1, g, lse.at[g + off_group, pl.ds(rows, rows)], ldst.at[g + off_group], to))

    def q_start(kinds, g):
        for kind in kinds:
            for copy in q_copies(kind, g):
                copy.start()

    def q_wait(kinds, g):
        for kind in kinds:
            for copy in q_copies(kind, g):
                copy.wait_recv()

    def start_own(g):
        q_start((1, 2, 0), g)

    def forward(g):
        q_wait((1, 2), g)
        q_start((3, 4, 5), g)

    def forward_diagonal(g):
        q_wait((3,), g)
        q_start((6,), g)

    def q_ready(g):
        q_wait((0, 4, 5, 6), g)

    def rs_start(stage, g):
        for copy in rs_copies(stage, g):
            copy.start()

    def rs_wait(stage, g):
        for copy in rs_copies(stage, g):
            copy.wait_recv()

    def kv_copy(b):
        slot = b % NBUF
        return pltpu.make_async_copy(c_ref.at[b], kv.at[slot], kv_sem.at[slot])

    def own_copies(lo, hi, k):
        return (pltpu.make_async_copy(ql_ref.at[lo:hi], ql.at[lo:hi, 0:8], q_sem.at[k]),
                pltpu.make_async_copy(qr_ref.at[lo // 2:hi // 2], qr.at[lo // 2:hi // 2, 0:8], q_sem.at[k + 1]))

    first_own, other_own = own_copies(0, 2 * G, 0), own_copies(2 * G, n_seq, 2)
    for copy in first_own + other_own:
        copy.start()
    for b in range(W):
        kv_copy(b).start()

    barrier = pltpu.get_barrier_semaphore()
    for device in (partner, neighbour(0, True), neighbour(0, False)):
        pl.semaphore_signal(barrier, inc=1, device_id=device, device_id_type=MESH)
    pl.semaphore_wait(barrier, 3)
    for copy in first_own:
        copy.wait()
    start_own(0)
    start_own(1)
    for copy in other_own:
        copy.wait()
    forward(0)
    start_own(2)
    forward(1)
    forward_diagonal(0)
    start_own(3)

    lane = lax.broadcasted_iota(jnp.int32, (8 * 8, 128), 1)

    def combine(stage, unit):
        rows, ref, lref = ((32, r1, rl1), (16, r2, rl2), (8, r3, rl3))[stage]
        g = unit // UNITS
        mine = lse[g, 0:rows]
        theirs = lref[g]
        for u in range(W):
            b = W * unit + u
            j = b % G
            merged, total = merge(o[b, 0:rows], column(mine, lane[0:rows], j),
                                  ref[b], column(theirs, lane[0:rows], j))
            if stage == 2:
                out_ref[jnp.maximum(b - W * OFF, 0)] = merged
            else:
                o[b, 0:rows] = merged
                mine = jnp.where(lane[0:rows] == j, total, mine)
        if stage != 2:
            lse[g, 0:rows] = mine

    def finish(t):
        for j in range(W):
            b = W * t + j
            o[b + W * OFF] = values([prob[(t + 2) % 2, j, i] for i in range(4)], kv.at[(b + NBUF) % NBUF])

    def begin(t):
        rows = lse[t // UNITS + off_group]
        for j in range(W):
            b = W * t + j
            p, total = softmax(scores(ql[b], qr[W // 2 * t + j % (W // 2), :, ROPE * (j // (W // 2)):ROPE * (j // (W // 2) + 1)],
                                      kv.at[b % NBUF]), lens_ref[b], me)
            for i in range(4):
                prob[t % 2, j, i] = p[i]
            rows = jnp.where(lane == b % G, total, rows)
        lse[t // UNITS + off_group] = rows

    def step(t, _):
        g = t // UNITS

        @pl.when(t % UNITS == 0)
        def _():
            @pl.when(g + AHEAD < n_groups)
            def _():
                start_own(g + AHEAD)

            @pl.when(g + 2 < n_groups)
            def _():
                forward(g + 2)

            @pl.when(g + 1 < n_groups)
            def _():
                forward_diagonal(g + 1)

            q_ready(g)

            @pl.when(g >= 2)
            def _():
                rs_wait(0, g - 2)

            @pl.when(g >= 3)
            def _():
                rs_start(1, g - 3)

            @pl.when(g >= 5)
            def _():
                rs_wait(1, g - 5)

            @pl.when(g >= 6)
            def _():
                rs_start(2, g - 6)

            @pl.when(g >= 8)
            def _():
                rs_wait(2, g - 8)

        @pl.when((t % UNITS == 1) & (g >= 1))
        def _():
            rs_start(0, g - 1)

        @pl.when(t + 1 < n_units)
        def _():
            for j in range(W):
                kv_copy(W * (t + 1) + j).start()
        for j in range(W):
            kv_copy(W * t + j).wait()
        combine(0, t - LAG1 + OFF)
        combine(1, t - LAG2 + OFF)
        combine(2, t - LAG3 + OFF)
        begin(t)
        finish(t - 1)
        return 0

    lax.fori_loop(0, n_units, step, 0)

    def combine_all(stage, lo, hi):
        def one(t, _):
            combine(stage, t + OFF)
            return 0
        lax.fori_loop(lo, hi, one, 0)

    last = n_groups - 1

    def merge_group(stage, g):
        rs_wait(stage, g)
        combine_all(stage, UNITS * g, UNITS * (g + 1))
        if stage < 2:
            rs_start(stage + 1, g)

    rs_start(1, last - 2)
    rs_start(2, last - 5)
    finish(n_units - 1)
    rs_start(0, last)
    for stage, back in ((1, 4), (0, 1), (1, 3), (0, 0), (2, 7), (1, 2), (2, 6), (2, 5), (1, 1), (2, 4), (2, 3), (1, 0),
                        (2, 2), (2, 1)):
        merge_group(stage, last - back)

    def sent(g, _):
        for kind in range(AG_KINDS // 2):
            for copy in q_copies(kind, g):
                copy.wait_send()
        for stage in range(3):
            for copy in rs_copies(stage, g):
                copy.wait_send()
        return 0

    lax.fori_loop(0, n_groups, sent, 0)
    merge_group(2, last)


def solution(mesh):
    def local(lens, q, cache):
        b, heads, k = q.shape
        r, page = cache.shape[1], cache.shape[3]
        lora = k - ROPE
        c = jnp.transpose(cache.reshape(b, r, page, k), (0, 2, 3, 1))
        groups = b // G
        q_latent = q[:, :, :lora]
        q_rotary = q[:, :, lora:].reshape(b // W, 2, W // 2, heads, ROPE).transpose(0, 2, 3, 1, 4)
        q_rotary = q_rotary.reshape(b // 2, heads, 2 * ROPE)
        pb = b + OFF * W
        pg = groups + OFF // UNITS
        bf, f4 = jnp.bfloat16, jnp.float32
        kinds = AG_KINDS + RS_KINDS
        return pl.pallas_call(
            functools.partial(kernel, b, lora),
            out_shape=jax.ShapeDtypeStruct((b, heads, lora), bf),
            in_specs=[pl.BlockSpec(memory_space=pltpu.SMEM)] + [pl.BlockSpec(memory_space=pl.ANY)] * 3,
            out_specs=pl.BlockSpec(memory_space=pltpu.VMEM),
            scratch_shapes=[
                pltpu.VMEM((NBUF, page, k, r), bf),
                pltpu.VMEM((b, 8 * heads, lora), bf), pltpu.VMEM((b // 2, 8 * heads, 2 * ROPE), bf),
                pltpu.VMEM((2, W, 4, 64, TILE), bf),
                pltpu.VMEM((pb, 64, lora), bf), pltpu.VMEM((pg, 64, 128), f4),
                pltpu.VMEM((pb, 32, lora), bf), pltpu.VMEM((pg, 32, 128), f4),
                pltpu.VMEM((pb, 16, lora), bf), pltpu.VMEM((pg, 16, 128), f4),
                pltpu.VMEM((pb, 8, lora), bf), pltpu.VMEM((pg, 8, 128), f4),
                pltpu.SemaphoreType.DMA((NBUF,)), pltpu.SemaphoreType.DMA((4,)),
                pltpu.SemaphoreType.DMA((kinds, groups)), pltpu.SemaphoreType.DMA((kinds, groups)),
            ],
            compiler_params=pltpu.CompilerParams(collective_id=0, has_side_effects=True,
                                                 vmem_limit_bytes=64 * 2 ** 20 - 2 ** 16),
            name="decode",
        )(lens, q_latent, q_rotary, c)

    f = jax.shard_map(local, mesh=mesh, in_specs=(P('dp'), P('dp', 'dcp', None), P('dp', None, 'dcp', None, None)),
                      out_specs=P('dp', 'dcp', None), check_vma=False)
    return lambda q, cache, lens: f(lens, q, cache)
```

```python
import functools

import jax
import jax.numpy as jnp
from jax import lax
from jax.experimental import pallas as pl
from jax.experimental.pallas import tpu as pltpu
from jax.sharding import PartitionSpec as P

ROPE = 64
QK_DIM = 192
SCALE = QK_DIM ** -0.5
MESH = pl.DeviceIdType.MESH

G = 8
W = 4
UNITS = G // W
AHEAD = 4
LAGS = (4, 9, 14)
TAIL = (4, 7, 10)
OFF = 14
NBUF = 3 * W
TILE = 256
LOG2E = 1.4426950408889634
AG_KINDS, RS_KINDS = 14, 6


def scores(ql, r, c):
    lora = 2 * TILE
    heads, rope = r.shape

    def rows(p, lo, hi):
        return jnp.concatenate([c[2 * p, lo:hi], c[2 * p + 1, lo:hi]], axis=1)

    ql = jnp.concatenate([ql] * 2, axis=0)
    z = jnp.zeros((heads, rope), jnp.bfloat16)
    qr = jnp.concatenate([jnp.concatenate([r if i == p else z for i in range(4)], axis=1)
                          for p in range(4)], axis=0)
    cr = jnp.concatenate([rows(p, lora, lora + rope) for p in range(4)], axis=0)
    rotary = jnp.dot(qr, cr, preferred_element_type=jnp.float32)
    out = []
    for p in range(4):
        v = jnp.dot(ql, rows(p, 0, lora), preferred_element_type=jnp.float32)[:heads]
        v = v + rotary[heads * p:heads * (p + 1)]
        out += [v[:, :128], v[:, 128:]]
    return out


def values(p, c):
    lora = 2 * TILE
    o = None
    for i in range(4):
        both = jnp.concatenate([c[2 * i, :lora], c[2 * i + 1, :lora]], axis=1)
        x = lax.dot_general(both, p[i], (((1,), (1,)), ((), ())), preferred_element_type=jnp.float32)
        o = x if o is None else o + x
    return o.astype(jnp.bfloat16).T


def softmax(s, length, d):
    lane = lax.broadcasted_iota(jnp.int32, s[0].shape, 1)
    s = [jnp.where(lane < lax.shift_right_arithmetic(length - 8 * d - i + 63, 6), v, -jnp.inf)
         for i, v in enumerate(s)]
    m = jnp.max(functools.reduce(jnp.maximum, s), axis=1, keepdims=True)
    m = jnp.where(m == -jnp.inf, 0.0, m)
    mc = m * (SCALE * LOG2E)
    p = [jnp.exp2(v * (SCALE * LOG2E) - mc) for v in s]
    l = jnp.sum(functools.reduce(jnp.add, p), axis=1, keepdims=True)
    has = l > 0.0
    safe = jnp.where(has, l, 1.0)
    r = jnp.where(has, 1.0 / safe, 0.0)
    lse = jnp.where(has, m * SCALE + jnp.log(safe), -jnp.inf)
    return [jnp.concatenate([p[2 * i] * r, p[2 * i + 1] * r], axis=1).astype(jnp.bfloat16) for i in range(4)], lse


def column(ref, lane, j):
    return jnp.max(jnp.where(lane == j, ref, -jnp.inf), axis=1, keepdims=True)


def merge(oa, la, ob, lb):
    top = jnp.maximum(la, lb)
    top = jnp.where(top == -jnp.inf, 0.0, top)
    wa, wb = jnp.exp(la - top), jnp.exp(lb - top)
    w = wa + wb
    has = w > 0.0
    safe = jnp.where(has, w, 1.0)
    inv = jnp.where(has, 1.0 / safe, 0.0)
    o = (wa * inv) * oa.astype(jnp.float32) + (wb * inv) * ob.astype(jnp.float32)
    return o.astype(jnp.bfloat16), jnp.where(has, top + jnp.log(safe), -jnp.inf)


def kernel(n_seq, lora, lens_ref, q_ref, c_ref, out_ref, kv, own, ql, qr, prob, o, lse, r1, rl1, r2, rl2, r3, rl3,
           kv_sem, q_sem, send_sem, recv_sem):
    n_groups, n_units = n_seq // G, n_seq // W
    off_group = OFF // UNITS
    me = lax.axis_index("dcp")
    dp = lax.axis_index("dp")
    y, x, core = me // 4, (me // 2) % 2, me % 2
    partner = (dp, y * 4 + x * 2 + (1 - core))
    diagonal = (dp, (1 - y) * 4 + (1 - x) * 2 + core)

    def neighbour(g, first):
        par = g % 2 if first else (g + 1) % 2
        return (dp, ((y + par) % 2) * 4 + ((x + 1 - par) % 2) * 2 + core)

    def remote(kind, g, src, dst, device):
        return pltpu.make_async_remote_copy(
            src_ref=src, dst_ref=dst, send_sem=send_sem.at[kind, g], recv_sem=recv_sem.at[kind, g],
            device_id=device, device_id_type=MESH)

    def q_blocks(g, block):
        return (ql.at[pl.ds(g * G, G), pl.ds(block * 8, 8)], qr.at[pl.ds(g * G // 2, G // 2), pl.ds(block * 8, 8)])

    def q_copies(kind, g):
        src, dst, to = ((0, 4, partner), (0, 2, neighbour(g, True)), (0, 1, neighbour(g, False)),
                        (2, 3, neighbour(g, False)), (2, 6, partner), (1, 5, partner), (3, 7, partner))[kind]
        return [remote(2 * kind + i, g, q_blocks(g, src)[i], q_blocks(g, dst)[i], to) for i in range(2)]

    def seqs(ref, g, lo, hi):
        return ref.at[pl.ds((g + off_group) * G, G), pl.ds(lo, hi - lo)]

    def rs_copies(stage, g):
        rows, dst, ldst, to = ((32, r1, rl1, partner), (16, r2, rl2, neighbour(g, True)),
                               (8, r3, rl3, neighbour(g, False)))[stage]
        kind = AG_KINDS + 2 * stage
        return (remote(kind, g, seqs(o, g, rows, 2 * rows), seqs(dst, g, 0, rows), to),
                remote(kind + 1, g, lse.at[g + off_group, pl.ds(rows, rows)], ldst.at[g + off_group], to))

    def q_start(kinds, g):
        for kind in kinds:
            for copy in q_copies(kind, g):
                copy.start()

    def q_wait(kinds, g):
        for kind in kinds:
            for copy in q_copies(kind, g):
                copy.wait_recv()

    def pack(g):
        for j in range(G):
            ql[g * G + j, 0:8] = own[g * G + j, :, 0:lora]
        for i in range(G // 2):
            b = g * G + i // (W // 2) * W + i % (W // 2)
            qr[g * G // 2 + i, 0:8] = jnp.concatenate([own[b, :, lora:], own[b + W // 2, :, lora:]], axis=1)

    def start_own(g):
        pack(g)
        q_start((1, 2, 0), g)

    def start_diagonal(g):
        for i in range(2):
            remote(6 + i, g, q_blocks(g, 0)[i], q_blocks(g, 3)[i], diagonal).start()

    def forward(g, kinds=(3, 4, 5)):
        q_wait((1, 2), g)
        q_start(kinds, g)

    def forward_diagonal(g):
        q_wait((3,), g)
        q_start((6,), g)

    def q_ready(g):
        q_wait((0, 4, 5, 6), g)

    def rs_start(stage, g):
        for copy in rs_copies(stage, g):
            copy.start()

    def rs_wait(stage, g):
        for copy in rs_copies(stage, g):
            copy.wait_recv()

    def kv_copy(b):
        slot = b % NBUF
        return pltpu.make_async_copy(c_ref.at[b], kv.at[slot], kv_sem.at[slot])

    first_own = pltpu.make_async_copy(q_ref.at[0:2 * G], own.at[0:2 * G], q_sem.at[0])
    other_own = pltpu.make_async_copy(q_ref.at[2 * G:n_seq], own.at[2 * G:n_seq], q_sem.at[1])
    first_own.start()
    other_own.start()
    for b in range(W):
        kv_copy(b).start()

    barrier = pltpu.get_barrier_semaphore()
    for device in (partner, diagonal, neighbour(0, True), neighbour(0, False)):
        pl.semaphore_signal(barrier, inc=1, device_id=device, device_id_type=MESH)
    pl.semaphore_wait(barrier, 4)
    first_own.wait()
    start_own(0)
    start_diagonal(0)
    start_own(1)
    other_own.wait()
    forward(0, (4, 5))
    start_own(2)
    forward(1)
    forward_diagonal(0)
    start_own(3)

    lane = lax.broadcasted_iota(jnp.int32, (8 * 8, 128), 1)

    def combine(stage, unit, count=1):
        rows, ref, lref = ((32, r1, rl1), (16, r2, rl2), (8, r3, rl3))[stage]
        g = unit // UNITS
        mine = lse[g, 0:rows]
        totals = mine
        theirs = lref[g]
        for u in range(W * count):
            b = W * unit + u
            j = b % G
            merged, total = merge(o[b, 0:rows], column(mine, lane[0:rows], j),
                                  ref[b], column(theirs, lane[0:rows], j))
            if stage == 2:
                out_ref[jnp.maximum(b - W * OFF, 0)] = merged
            else:
                o[b, 0:rows] = merged
                totals = jnp.where(lane[0:rows] == j, total, totals)
        if stage != 2:
            lse[g, 0:rows] = totals

    def finish(t):
        for j in range(W):
            b = W * t + j
            o[b + W * OFF] = values([prob[(t + 2) % 2, j, i] for i in range(4)], kv.at[(b + NBUF) % NBUF])

    def begin(t):
        rows = lse[t // UNITS + off_group]
        for j in range(W):
            b = W * t + j
            p, total = softmax(scores(ql[b], qr[W // 2 * t + j % (W // 2), :, ROPE * (j // (W // 2)):ROPE * (j // (W // 2) + 1)],
                                      kv.at[b % NBUF]), lens_ref[b], me)
            for i in range(4):
                prob[t % 2, j, i] = p[i]
            rows = jnp.where(lane == b % G, total, rows)
        lse[t // UNITS + off_group] = rows

    def step(t, _):
        g = t // UNITS

        def exchange(parity):
            for stage in (1, 0):
                if LAGS[stage] % UNITS == parity:
                    older = LAGS[stage] // UNITS + 1

                    @pl.when(g >= older)
                    def _(stage=stage, older=older):
                        rs_start(stage + 1, g - older)
            for stage in range(3):
                if LAGS[stage] % UNITS == parity:
                    back = LAGS[stage] // UNITS

                    @pl.when(g >= back)
                    def _(stage=stage, back=back):
                        rs_wait(stage, g - back)

        @pl.when(t % UNITS == 0)
        def _():
            q_ready(g)
            exchange(0)

        @pl.when(t % UNITS == 1)
        def _():
            @pl.when(g >= 1)
            def _():
                rs_start(0, g - 1)

            @pl.when(g + AHEAD < n_groups)
            def _():
                start_own(g + AHEAD)

            @pl.when(g + 2 < n_groups)
            def _():
                forward(g + 2)

            @pl.when(g + 1 < n_groups)
            def _():
                forward_diagonal(g + 1)

            exchange(1)

        @pl.when(t + 1 < n_units)
        def _():
            for j in range(W):
                kv_copy(W * (t + 1) + j).start()
        for j in range(W):
            kv_copy(W * t + j).wait()
        for stage in range(3):
            combine(stage, t - LAGS[stage] + OFF)
        begin(t)
        finish(t - 1)
        return 0

    lax.fori_loop(0, n_units, step, 0)

    def combine_all(stage, lo, hi):
        def one(t, _):
            combine(stage, t + OFF)
            return 0
        lax.fori_loop(lo, hi, one, 0)

    last = n_groups - 1
    rest = []
    for stage in range(3):
        unit = n_units - LAGS[stage]
        if unit % UNITS:
            combine_all(stage, unit, unit + 1)
        g = unit // UNITS - (unit % UNITS == 0)
        if stage < 2:
            rs_start(stage + 1, g)
        rest += [(UNITS * i + TAIL[stage], stage, i) for i in range(g + 1, n_groups)]

    def merge_group(stage, g):
        rs_wait(stage, g)
        combine(stage, UNITS * g + OFF, UNITS)
        if stage < 2:
            rs_start(stage + 1, g)

    finish(n_units - 1)
    rs_start(0, last)
    for _, stage, g in sorted(rest)[:-1]:
        merge_group(stage, g)

    def sent(g, _):
        for kind in range(AG_KINDS // 2):
            for copy in q_copies(kind, g):
                copy.wait_send()
        for stage in range(3):
            for copy in rs_copies(stage, g):
                copy.wait_send()
        return 0

    lax.fori_loop(0, n_groups, sent, 0)
    merge_group(2, last)


def solution(mesh):
    def local(lens, q, cache):
        b, heads, k = q.shape
        r, page = cache.shape[1], cache.shape[3]
        lora = k - ROPE
        c = jnp.transpose(cache.reshape(b, r, page, k), (0, 2, 3, 1))
        groups = b // G
        pb = b + OFF * W
        pg = groups + OFF // UNITS
        bf, f4 = jnp.bfloat16, jnp.float32
        kinds = AG_KINDS + RS_KINDS
        return pl.pallas_call(
            functools.partial(kernel, b, lora),
            out_shape=jax.ShapeDtypeStruct((b, heads, lora), bf),
            in_specs=[pl.BlockSpec(memory_space=pltpu.SMEM)] + [pl.BlockSpec(memory_space=pl.ANY)] * 2,
            out_specs=pl.BlockSpec(memory_space=pltpu.VMEM),
            scratch_shapes=[
                pltpu.VMEM((NBUF, page, k, r), bf),
                pltpu.VMEM((b, heads, k), bf),
                pltpu.VMEM((b, 8 * heads, lora), bf), pltpu.VMEM((b // 2, 8 * heads, 2 * ROPE), bf),
                pltpu.VMEM((2, W, 4, 64, TILE), bf),
                pltpu.VMEM((pb, 64, lora), bf), pltpu.VMEM((pg, 64, 128), f4),
                pltpu.VMEM((pb, 32, lora), bf), pltpu.VMEM((pg, 32, 128), f4),
                pltpu.VMEM((pb, 16, lora), bf), pltpu.VMEM((pg, 16, 128), f4),
                pltpu.VMEM((pb, 8, lora), bf), pltpu.VMEM((pg, 8, 128), f4),
                pltpu.SemaphoreType.DMA((NBUF,)), pltpu.SemaphoreType.DMA((2,)),
                pltpu.SemaphoreType.DMA((kinds, groups)), pltpu.SemaphoreType.DMA((kinds, groups)),
            ],
            compiler_params=pltpu.CompilerParams(collective_id=0, has_side_effects=True,
                                                 vmem_limit_bytes=64 * 2 ** 20 - 2 ** 16),
            name="decode",
        )(lens, q, c)

    f = jax.shard_map(local, mesh=mesh, in_specs=(P('dp'), P('dp', 'dcp', None), P('dp', None, 'dcp', None, None)),
                      out_specs=P('dp', 'dcp', None), check_vma=False)
    return lambda q, cache, lens: f(lens, q, cache)
```

```python
import functools

import jax
import jax.numpy as jnp
from jax import lax
from jax.experimental import pallas as pl
from jax.experimental.pallas import tpu as pltpu
from jax.sharding import PartitionSpec as P

ROPE = 64
QK_DIM = 192
SCALE = QK_DIM ** -0.5
MESH = pl.DeviceIdType.MESH

G = 8
W = 4
UNITS = G // W
AHEAD = 6
LAGS = (4, 9, 14)
TAIL = (4, 7, 10)
OFF = 14
NBUF = 3 * W
TILE = 256
LOG2E = 1.4426950408889634
AG_KINDS, RS_KINDS = 14, 6


def scores(ql, r, c):
    lora = 2 * TILE
    heads, rope = r.shape

    def rows(p, lo, hi):
        return jnp.concatenate([c[2 * p, lo:hi], c[2 * p + 1, lo:hi]], axis=1)

    ql = jnp.concatenate([ql] * 2, axis=0)
    z = jnp.zeros((heads, rope), jnp.bfloat16)
    qr = jnp.concatenate([jnp.concatenate([r if i == p else z for i in range(4)], axis=1)
                          for p in range(4)], axis=0)
    cr = jnp.concatenate([rows(p, lora, lora + rope) for p in range(4)], axis=0)
    rotary = jnp.dot(qr, cr, preferred_element_type=jnp.float32)
    out = []
    for p in range(4):
        v = jnp.dot(ql, rows(p, 0, lora), preferred_element_type=jnp.float32)[:heads]
        v = v + rotary[heads * p:heads * (p + 1)]
        out += [v[:, :128], v[:, 128:]]
    return out


def values(p, c):
    lora = 2 * TILE
    o = None
    for i in range(4):
        both = jnp.concatenate([c[2 * i, :lora], c[2 * i + 1, :lora]], axis=1)
        x = lax.dot_general(both, p[i], (((1,), (1,)), ((), ())), preferred_element_type=jnp.float32)
        o = x if o is None else o + x
    return o.astype(jnp.bfloat16).T


def softmax(s, length, d):
    lane = lax.broadcasted_iota(jnp.int32, s[0].shape, 1)
    s = [jnp.where(lane < lax.shift_right_arithmetic(length - 8 * d - i + 63, 6), v, -jnp.inf)
         for i, v in enumerate(s)]
    m = jnp.max(functools.reduce(jnp.maximum, s), axis=1, keepdims=True)
    m = jnp.where(m == -jnp.inf, 0.0, m)
    mc = m * (SCALE * LOG2E)
    p = [jnp.exp2(v * (SCALE * LOG2E) - mc) for v in s]
    l = jnp.sum(functools.reduce(jnp.add, p), axis=1, keepdims=True)
    has = l > 0.0
    safe = jnp.where(has, l, 1.0)
    r = jnp.where(has, 1.0 / safe, 0.0)
    lse = jnp.where(has, m * SCALE + jnp.log(safe), -jnp.inf)
    return [jnp.concatenate([p[2 * i] * r, p[2 * i + 1] * r], axis=1).astype(jnp.bfloat16) for i in range(4)], lse


def column(ref, lane, j):
    return jnp.max(jnp.where(lane == j, ref, -jnp.inf), axis=1, keepdims=True)


def merge(oa, la, ob, lb):
    top = jnp.maximum(la, lb)
    top = jnp.where(top == -jnp.inf, 0.0, top)
    wa, wb = jnp.exp(la - top), jnp.exp(lb - top)
    w = wa + wb
    has = w > 0.0
    safe = jnp.where(has, w, 1.0)
    inv = jnp.where(has, 1.0 / safe, 0.0)
    o = (wa * inv) * oa.astype(jnp.float32) + (wb * inv) * ob.astype(jnp.float32)
    return o.astype(jnp.bfloat16), jnp.where(has, top + jnp.log(safe), -jnp.inf)


def kernel(n_seq, lora, lens_ref, q_ref, c_ref, out_ref, kv, own, ql, qr, prob, o, lse, r1, rl1, r2, rl2, r3, rl3,
           kv_sem, q_sem, send_sem, recv_sem):
    n_groups, n_units = n_seq // G, n_seq // W
    off_group = OFF // UNITS
    me = lax.axis_index("dcp")
    dp = lax.axis_index("dp")
    y, x, core = me // 4, (me // 2) % 2, me % 2
    partner = (dp, y * 4 + x * 2 + (1 - core))
    diagonal = (dp, (1 - y) * 4 + (1 - x) * 2 + core)

    def neighbour(g, first):
        par = g % 2 if first else (g + 1) % 2
        return (dp, ((y + par) % 2) * 4 + ((x + 1 - par) % 2) * 2 + core)

    def remote(kind, g, src, dst, device):
        return pltpu.make_async_remote_copy(
            src_ref=src, dst_ref=dst, send_sem=send_sem.at[kind, g], recv_sem=recv_sem.at[kind, g],
            device_id=device, device_id_type=MESH)

    def q_blocks(g, block):
        return (ql.at[pl.ds(g * G, G), pl.ds(block * 8, 8)], qr.at[pl.ds(g * G // 2, G // 2), pl.ds(block * 8, 8)])

    def q_copies(kind, g):
        src, dst, to = ((0, 4, partner), (0, 2, neighbour(g, True)), (0, 1, neighbour(g, False)),
                        (2, 3, neighbour(g, False)), (2, 6, partner), (1, 5, partner), (3, 7, partner))[kind]
        return [remote(2 * kind + i, g, q_blocks(g, src)[i], q_blocks(g, dst)[i], to) for i in range(2)]

    def seqs(ref, g, lo, hi):
        return ref.at[pl.ds((g + off_group) * G, G), pl.ds(lo, hi - lo)]

    def rs_copies(stage, g):
        rows, dst, ldst, to = ((32, r1, rl1, partner), (16, r2, rl2, neighbour(g, True)),
                               (8, r3, rl3, neighbour(g, False)))[stage]
        kind = AG_KINDS + 2 * stage
        return (remote(kind, g, seqs(o, g, rows, 2 * rows), seqs(dst, g, 0, rows), to),
                remote(kind + 1, g, lse.at[g + off_group, pl.ds(rows, rows)], ldst.at[g + off_group], to))

    def q_start(kinds, g):
        for kind in kinds:
            for copy in q_copies(kind, g):
                copy.start()

    def q_wait(kinds, g):
        for kind in kinds:
            for copy in q_copies(kind, g):
                copy.wait_recv()

    def pack(g):
        for j in range(G):
            ql[g * G + j, 0:8] = own[g * G + j, :, 0:lora]
        for i in range(G // 2):
            b = g * G + i // (W // 2) * W + i % (W // 2)
            qr[g * G // 2 + i, 0:8] = jnp.concatenate([own[b, :, lora:], own[b + W // 2, :, lora:]], axis=1)

    def start_own(g):
        pack(g)
        q_start((1, 2, 0), g)

    def start_diagonal(g):
        for i in range(2):
            remote(6 + i, g, q_blocks(g, 0)[i], q_blocks(g, 3)[i], diagonal).start()

    def forward(g, kinds=(3, 4, 5)):
        q_wait((1, 2), g)
        q_start(kinds, g)

    def forward_diagonal(g):
        q_wait((3,), g)
        q_start((6,), g)

    def q_ready(g):
        q_wait((0, 4, 5, 6), g)

    def rs_start(stage, g):
        for copy in rs_copies(stage, g):
            copy.start()

    def rs_wait(stage, g):
        for copy in rs_copies(stage, g):
            copy.wait_recv()

    def kv_copy(b):
        slot = b % NBUF
        return pltpu.make_async_copy(c_ref.at[b], kv.at[slot], kv_sem.at[slot])

    first_own = pltpu.make_async_copy(q_ref.at[0:2 * G], own.at[0:2 * G], q_sem.at[0])
    other_own = pltpu.make_async_copy(q_ref.at[2 * G:n_seq], own.at[2 * G:n_seq], q_sem.at[1])
    first_own.start()
    other_own.start()
    for b in range(W):
        kv_copy(b).start()

    barrier = pltpu.get_barrier_semaphore()
    for device in (partner, diagonal, neighbour(0, True), neighbour(0, False)):
        pl.semaphore_signal(barrier, inc=1, device_id=device, device_id_type=MESH)
    pl.semaphore_wait(barrier, 4)
    first_own.wait()
    start_own(0)
    start_diagonal(0)
    start_own(1)
    other_own.wait()
    forward(0, (4, 5))
    start_own(2)
    forward(1)
    forward_diagonal(0)
    start_own(3)
    start_own(4)
    start_own(5)

    lane = lax.broadcasted_iota(jnp.int32, (8 * 8, 128), 1)

    def combine(stage, unit, count=1):
        rows, ref, lref = ((32, r1, rl1), (16, r2, rl2), (8, r3, rl3))[stage]
        g = unit // UNITS
        mine = lse[g, 0:rows]
        totals = mine
        theirs = lref[g]
        for u in range(W * count):
            b = W * unit + u
            j = b % G
            merged, total = merge(o[b, 0:rows], column(mine, lane[0:rows], j),
                                  ref[b], column(theirs, lane[0:rows], j))
            if stage == 2:
                out_ref[jnp.maximum(b - W * OFF, 0)] = merged
            else:
                o[b, 0:rows] = merged
                totals = jnp.where(lane[0:rows] == j, total, totals)
        if stage != 2:
            lse[g, 0:rows] = totals

    def finish(t):
        for j in range(W):
            b = W * t + j
            o[b + W * OFF] = values([prob[(t + 2) % 2, j, i] for i in range(4)], kv.at[(b + NBUF) % NBUF])

    def begin(t):
        rows = lse[t // UNITS + off_group]
        for j in range(W):
            b = W * t + j
            p, total = softmax(scores(ql[b], qr[W // 2 * t + j % (W // 2), :, ROPE * (j // (W // 2)):ROPE * (j // (W // 2) + 1)],
                                      kv.at[b % NBUF]), lens_ref[b], me)
            for i in range(4):
                prob[t % 2, j, i] = p[i]
            rows = jnp.where(lane == b % G, total, rows)
        lse[t // UNITS + off_group] = rows

    def step(t, _):
        g = t // UNITS

        @pl.when(t + 1 < n_units)
        def _():
            for j in range(W):
                kv_copy(W * (t + 1) + j).start()

        def exchange(parity):
            for stage in (1, 0):
                if LAGS[stage] % UNITS == parity:
                    older = LAGS[stage] // UNITS + 1

                    @pl.when(g >= older)
                    def _(stage=stage, older=older):
                        rs_start(stage + 1, g - older)
            for stage in range(3):
                if LAGS[stage] % UNITS == parity:
                    back = LAGS[stage] // UNITS

                    @pl.when(g >= back)
                    def _(stage=stage, back=back):
                        rs_wait(stage, g - back)

        @pl.when(t % UNITS == 0)
        def _():
            q_ready(g)
            exchange(0)

        @pl.when(t % UNITS == 1)
        def _():
            @pl.when(g >= 1)
            def _():
                rs_start(0, g - 1)

            @pl.when(g + AHEAD < n_groups)
            def _():
                start_own(g + AHEAD)

            @pl.when(g + 2 < n_groups)
            def _():
                forward(g + 2)

            @pl.when(g + 1 < n_groups)
            def _():
                forward_diagonal(g + 1)

            exchange(1)

        for j in range(W):
            kv_copy(W * t + j).wait()
        for stage in range(3):
            combine(stage, t - LAGS[stage] + OFF)
        begin(t)
        finish(t - 1)
        return 0

    lax.fori_loop(0, n_units, step, 0)

    def combine_all(stage, lo, hi):
        def one(t, _):
            combine(stage, t + OFF)
            return 0
        lax.fori_loop(lo, hi, one, 0)

    last = n_groups - 1
    rest = []
    for stage in range(3):
        unit = n_units - LAGS[stage]
        if unit % UNITS:
            combine_all(stage, unit, unit + 1)
        g = unit // UNITS - (unit % UNITS == 0)
        if stage < 2:
            rs_start(stage + 1, g)
        rest += [(UNITS * i + TAIL[stage], stage, i) for i in range(g + 1, n_groups)]

    def merge_group(stage, g):
        rs_wait(stage, g)
        combine(stage, UNITS * g + OFF, UNITS)
        if stage < 2:
            rs_start(stage + 1, g)

    finish(n_units - 1)
    rs_start(0, last)
    for _, stage, g in sorted(rest)[:-1]:
        merge_group(stage, g)

    def sent(g, _):
        for kind in range(AG_KINDS // 2):
            for copy in q_copies(kind, g):
                copy.wait_send()
        for stage in range(3):
            for copy in rs_copies(stage, g):
                copy.wait_send()
        return 0

    lax.fori_loop(0, n_groups, sent, 0)
    merge_group(2, last)


def solution(mesh):
    def local(lens, q, cache):
        b, heads, k = q.shape
        r, page = cache.shape[1], cache.shape[3]
        lora = k - ROPE
        c = jnp.transpose(cache.reshape(b, r, page, k), (0, 2, 3, 1))
        groups = b // G
        pb = b + OFF * W
        pg = groups + OFF // UNITS
        bf, f4 = jnp.bfloat16, jnp.float32
        kinds = AG_KINDS + RS_KINDS
        return pl.pallas_call(
            functools.partial(kernel, b, lora),
            out_shape=jax.ShapeDtypeStruct((b, heads, lora), bf),
            in_specs=[pl.BlockSpec(memory_space=pltpu.SMEM)] + [pl.BlockSpec(memory_space=pl.ANY)] * 2,
            out_specs=pl.BlockSpec(memory_space=pltpu.VMEM),
            scratch_shapes=[
                pltpu.VMEM((NBUF, page, k, r), bf),
                pltpu.VMEM((b, heads, k), bf),
                pltpu.VMEM((b, 8 * heads, lora), bf), pltpu.VMEM((b // 2, 8 * heads, 2 * ROPE), bf),
                pltpu.VMEM((2, W, 4, 64, TILE), bf),
                pltpu.VMEM((pb, 64, lora), bf), pltpu.VMEM((pg, 64, 128), f4),
                pltpu.VMEM((pb, 32, lora), bf), pltpu.VMEM((pg, 32, 128), f4),
                pltpu.VMEM((pb, 16, lora), bf), pltpu.VMEM((pg, 16, 128), f4),
                pltpu.VMEM((pb, 8, lora), bf), pltpu.VMEM((pg, 8, 128), f4),
                pltpu.SemaphoreType.DMA((NBUF,)), pltpu.SemaphoreType.DMA((2,)),
                pltpu.SemaphoreType.DMA((kinds, groups)), pltpu.SemaphoreType.DMA((kinds, groups)),
            ],
            compiler_params=pltpu.CompilerParams(collective_id=0, has_side_effects=True,
                                                 vmem_limit_bytes=64 * 2 ** 20 - 2 ** 16),
            name="decode",
        )(lens, q, c)

    f = jax.shard_map(local, mesh=mesh, in_specs=(P('dp'), P('dp', 'dcp', None), P('dp', None, 'dcp', None, None)),
                      out_specs=P('dp', 'dcp', None), check_vma=False)
    return lambda q, cache, lens: f(lens, q, cache)
```
